512 devices in a mesh: replica: 2 (over y), kv: 16 (over z), head: 8 (over x), sub: 2 (over core).
Axes of the slice: x: 8, y: 2, z: 16, core: 2. Of those that a mesh axis runs over, the one named last changes fastest.
The devices are a block of a 8x8x16 slice.
Arguments:
- queries: bfloat16 [1024, 64, 128], P(('replica', 'kv'), 'head'), parts along dimension 0, may hold values from -12 to 12
- sys_keys: bfloat16 [16, 4096, 128], P(('replica', 'head'), ('kv', 'sub')), parts along dimension 0, may hold values from -5 to 5
- sys_values: bfloat16 [16, 4096, 128], P(('replica', 'head'), ('kv', 'sub')), parts along dimension 0, may hold values from -6 to 6
- task_keys: bfloat16 [32, 8, 4096, 128], P(('replica', 'kv'), 'head', 'sub'), parts along dimension 0, may hold values from -5 to 5
- task_values: bfloat16 [32, 8, 4096, 128], P(('replica', 'kv'), 'head', 'sub'), parts along dimension 0, may hold values from -6 to 6
- suffix_keys: bfloat16 [1024, 8, 512, 128], P(('replica', 'kv', 'sub'), 'head'), parts along dimension 0, may hold values from -5 to 5
- suffix_values: bfloat16 [1024, 8, 512, 128], P(('replica', 'kv', 'sub'), 'head'), parts along dimension 0, may hold values from -6 to 6
- task_ids: int32 [1024], P(('replica', 'kv')), parts along dimension 0, may hold values from 0 to 15, as said below
- suffix_len: int32 [1024], P(('replica', 'kv', 'sub')), parts along dimension 0, may hold values from 256 to 512, as said below
Outputs:
- attended: bfloat16 [1024, 64, 128], P(('replica', 'kv', 'sub'), 'head'), parts along dimension 0
The draws below stay inside these ranges and needn't reach their ends.
There are 2 independent parts, one for each index of `replica`. The reference program is written for one: setup_inputs(seed, part) draws one part's arguments, and reference() takes and returns one part's arrays. A program takes and returns all parts, laid end to end along the dimension named above; each array names one. Nothing has to cross between parts.
Inputs may be any that keep to these rules, and one draw needn't show every extreme that they name: `task_ids`: task t's prefix is task_keys[t]. The rows 2 * 16 * p to 2 * 16 * (p + 1) - 1 form aligned blocks; in each block no task is named more than 8 times, and one task, the same for all blocks, is named exactly 8 times in every block. `suffix_len`: each aligned block of 16 rows holds one length equal to 512.
All inputs are finite; a program needn't handle non-finite values.
Results may differ from the reference program's by a relative error of at most 0.005.
Values may be sent and summed in bfloat16 or wider, within the bound.
A program may use at most 64 MiB of HBM per device.

```python
import math
import jax
import jax.numpy as jnp
from jax import lax

QH = 64
KVH = 8
HD = 128
SEQ_DEV = 16
TASK = 4096
SUF = 512
CAP = 8
SEQS = 512
SYS = 4096
TASKS = 16


def draw_keys_like(key, tag_value, full_shape):
    own_key = jax.random.fold_in(key, tag_value)
    first_key = jax.random.fold_in(own_key, 0)
    drawn = jnp.clip(jax.random.normal(first_key, full_shape, jnp.float32), -5.0, 5.0)
    return drawn.astype(jnp.bfloat16)


def draw_queries(key, part):
    own_key = jax.random.fold_in(key, 11)
    first_key = jax.random.fold_in(own_key, 0)
    drawn = jax.random.normal(first_key, (SEQS, QH, HD), jnp.float32) * 2.5
    return jnp.clip(drawn, -12.0, 12.0).astype(jnp.bfloat16)


def draw_sys_keys(key, part):
    return draw_keys_like(key, 31, (KVH, SYS, HD))


def draw_task_keys(key, part):
    return draw_keys_like(key, 37, (TASKS, KVH, TASK, HD))


def draw_suffix_keys(key, part):
    return draw_keys_like(key, 41, (SEQS, KVH, SUF, HD))


def draw_task_ids(key, part):
    own_key = jax.random.fold_in(key, 23)
    pair_count = SEQS // (2 * SEQ_DEV)
    busiest = jax.random.randint(jax.random.fold_in(own_key, 1), (), 0, TASKS)
    tickets = jnp.repeat(jnp.arange(TASKS - 1, dtype=jnp.int32), CAP)
    others = tickets + (tickets >= busiest).astype(jnp.int32)

    def one_pair(pair_index):
        pair_key = jax.random.fold_in(own_key, pair_index + 2)
        chosen = jax.random.permutation(jax.random.fold_in(pair_key, 0), others)[:2 * SEQ_DEV - CAP]
        joined = jnp.concatenate([chosen, jnp.full((CAP,), busiest, jnp.int32)])
        return jax.random.permutation(jax.random.fold_in(pair_key, 1), joined)
    return jax.vmap(one_pair)(jnp.arange(pair_count, dtype=jnp.int32)).reshape(SEQS).astype(jnp.int32)


def draw_suffix_len(key, part):
    own_key = jax.random.fold_in(key, 29)
    lengths = jax.random.randint(jax.random.fold_in(own_key, 1), (SEQS,), SUF // 2, SUF + 1)
    picked = jax.random.randint(jax.random.fold_in(own_key, 2), (SEQS // SEQ_DEV,), 0, SEQ_DEV)
    within = jnp.arange(SEQS, dtype=jnp.int32) % SEQ_DEV
    return jnp.where(within == jnp.repeat(picked, SEQ_DEV), SUF, lengths).astype(jnp.int32)


def level_of(rng, extent, pieces, least, high):
    def one(dim, blocks):
        draws = jax.random.uniform(jax.random.fold_in(jax.random.fold_in(rng, 6), dim), (blocks,), jnp.float32, least / len(pieces), high / len(pieces))
        return jnp.repeat(jnp.exp(draws), extent[dim] // blocks).reshape((-1,) + (1,) * (len(extent) - dim - 1))

    gain = one(*pieces[0])
    for cut in pieces[1:]:
        gain = gain * one(*cut)
    return gain


def bell_draw(stream_key, shape, deviation, most, cuts=(), kind=jnp.bfloat16):
    level = level_of(stream_key, shape, cuts, -0.22, 0.18) if cuts else 1.0
    entries = jax.random.normal(stream_key, shape, jnp.float32) * deviation * level
    return jnp.minimum(jnp.maximum(entries, -most), most).astype(kind)


def setup_inputs(seed: int = 0, part: int = 0) -> dict:
    key_of = jax.random.split(jax.random.key(seed), 10)
    part_keys = jax.random.split(jax.random.fold_in(key_of[9], part), 10)
    return {
        "queries": draw_queries(jax.random.fold_in(jax.random.fold_in(key_of[9], part), 71), part),
        "sys_keys": draw_sys_keys(jax.random.fold_in(jax.random.fold_in(key_of[9], part), 71), part),
        "sys_values": bell_draw(part_keys[2], (KVH, SYS, HD), 1.0, 6.0, ((0, 8), (1, 32))),
        "task_keys": draw_task_keys(jax.random.fold_in(jax.random.fold_in(key_of[9], part), 71), part),
        "task_values": bell_draw(part_keys[4], (TASKS, KVH, TASK, HD), 1.0, 6.0, ((0, 16), (1, 8), (2, 2))),
        "suffix_keys": draw_suffix_keys(jax.random.fold_in(jax.random.fold_in(key_of[9], part), 71), part),
        "suffix_values": bell_draw(part_keys[6], (SEQS, KVH, SUF, HD), 1.0, 6.0, ((0, 32), (1, 8))),
        "task_ids": draw_task_ids(jax.random.fold_in(jax.random.fold_in(key_of[9], part), 71), part),
        "suffix_len": draw_suffix_len(jax.random.fold_in(jax.random.fold_in(key_of[9], part), 71), part),
    }


NEGATIVE = -1e+30

def level_partial(query_rows, level_keys, level_values, usable):
    score_scale = 1.0 / math.sqrt(HD)
    scores = jnp.einsum('kgd,kld->kgl', query_rows, level_keys.astype(jnp.float32)) * score_scale
    scores = jnp.where(usable[None, None, :], scores, NEGATIVE)
    maxima = lax.optimization_barrier(jnp.max(scores, axis=2))
    weights = jnp.where(usable[None, None, :], jnp.exp(scores - maxima[:, :, None]), 0.0)
    totals = lax.optimization_barrier(jnp.sum(weights, axis=2))
    rounded = lax.optimization_barrier(weights.astype(jnp.bfloat16))
    numerator = jnp.einsum('kgl,kld->kgd', rounded.astype(jnp.float32), level_values.astype(jnp.float32))
    return (maxima, totals, numerator)

def reference(queries, sys_keys, sys_values, task_keys, task_values, suffix_keys, suffix_values, task_ids, suffix_len):
    group_size = QH // KVH
    every_system = jnp.ones((SYS,), dtype=jnp.bool_)
    every_task = jnp.ones((TASK,), dtype=jnp.bool_)
    positions = jnp.arange(SUF, dtype=jnp.int32)

    def per_sequence(packed):
        query_row, task_index, length, own_keys, own_values = packed
        query_rows = query_row.astype(jnp.float32).reshape(KVH, group_size, HD)
        chosen_keys = lax.dynamic_index_in_dim(task_keys, task_index.astype(jnp.int32), 0, keepdims=False)
        chosen_values = lax.dynamic_index_in_dim(task_values, task_index.astype(jnp.int32), 0, keepdims=False)
        system_level = level_partial(query_rows, sys_keys, sys_values, every_system)
        task_level = level_partial(query_rows, chosen_keys, chosen_values, every_task)
        suffix_level = level_partial(query_rows, own_keys, own_values, positions < length)
        highest = jnp.maximum(jnp.maximum(system_level[0], task_level[0]), suffix_level[0])
        system_factor = jnp.exp(system_level[0] - highest)
        task_factor = jnp.exp(task_level[0] - highest)
        suffix_factor = jnp.exp(suffix_level[0] - highest)
        totals = system_level[1] * system_factor + task_level[1] * task_factor + suffix_level[1] * suffix_factor
        numerator = system_level[2] * system_factor[:, :, None] + task_level[2] * task_factor[:, :, None] + suffix_level[2] * suffix_factor[:, :, None]
        return (numerator / totals[:, :, None]).reshape(QH, HD).astype(jnp.bfloat16)
    return lax.map(per_sequence, (queries, task_ids, suffix_len, suffix_keys, suffix_values))
```

```python
import functools
import math

import jax
import jax.numpy as jnp
from jax import lax
from jax.experimental import pallas as pl
from jax.experimental.pallas import tpu as pltpu
from jax.sharding import PartitionSpec as P

CAP = 8
NEGATIVE = -1e30
MESH = pl.DeviceIdType.MESH
F32 = jnp.float32
BF16 = jnp.bfloat16


def nt_dot(a, b):
    return lax.dot_general(a, b, (((1,), (1,)), ((), ())), preferred_element_type=F32)


def nn_dot(a, b):
    return lax.dot_general(a, b, (((1,), (0,)), ((), ())), preferred_element_type=F32)


def iota(shape, dim):
    return lax.broadcasted_iota(jnp.int32, shape, dim)


def kernel(
    n,
    heads,
    q_hbm,
    sk_hbm,
    sv_hbm,
    tk_hbm,
    tv_hbm,
    uk_hbm,
    uv_hbm,
    ids_ref,
    len_ref,
    out_ref,
    qv,
    kall,
    vall,
    tk,
    tv,
    uk,
    uv,
    qs,
    qr,
    rs,
    rr,
    ss,
    sr,
    gmat,
    scores,
    sys_m,
    sys_l,
    sys_acc,
    suf_l,
    suf_o,
    xs,
    xr,
    local_sem,
    ring_send,
    ring_recv,
    q_send,
    q_recv,
    r_send,
    r_recv,
    s_send,
    s_recv,
    t_send,
    t_recv,
    x_send,
    x_recv,
):
    z = lax.axis_index("kv")
    c = lax.axis_index("sub")
    half = n // 2
    rows, hd = q_hbm.shape
    pair = rows // heads
    own = rows // 2
    own_seqs = uk_hbm.shape[0]
    suf = uk_hbm.shape[1]
    task_half = tk_hbm.shape[0]
    slots = CAP // 2
    hb = slots * heads
    per = hd // hb
    unit = math.log2(math.e) / math.sqrt(hd)

    order = [0]
    for d in range(1, half):
        order += [d, n - d]
    order.append(half)
    place = {o: k for k, o in enumerate(order)}

    def at(offset):
        return place[offset % n]

    def kv_dev(offset):
        return {"kv": lax.rem(z + (offset % n), n)}

    partner = {"sub": 1 - c}

    loads = []
    for i, (src, dst) in enumerate(
        (
            (q_hbm, qv),
            (sk_hbm, kall.at[0]),
            (sv_hbm, vall.at[0]),
            (uk_hbm, uk),
            (uv_hbm, uv),
            (tk_hbm, tk.at[0]),
            (tv_hbm, tv.at[0]),
        )
    ):
        copy = pltpu.make_async_copy(src, dst, local_sem.at[i])
        copy.start()
        loads.append(copy)

    barrier = pltpu.get_barrier_semaphore()
    pl.semaphore_signal(barrier, inc=1, device_id=partner, device_id_type=MESH)
    for o in order[1:]:
        pl.semaphore_signal(barrier, inc=1, device_id=kv_dev(o), device_id_type=MESH)

    ids_row = ids_ref[...].astype(F32)
    ids_b = jnp.broadcast_to(ids_row, (pair, pair))
    eye = iota((pair, pair), 0) == iota((pair, pair), 1)
    ids_col = jnp.sum(jnp.where(eye, ids_b, 0.0), axis=1, keepdims=True)
    before = iota((pair, pair), 0) < iota((pair, pair), 1)
    same = jnp.logical_and(ids_col == ids_b, before)
    rank_row = jnp.sum(jnp.where(same, 1.0, 0.0), axis=0, keepdims=True)
    code_row = ids_row * CAP + rank_row
    code_b = jnp.broadcast_to(code_row, (pair, pair))
    spread = (iota((rows, pair), 0) // heads == iota((rows, pair), 1))
    code_col = jnp.sum(
        jnp.where(spread, jnp.broadcast_to(code_row, (rows, pair)), 0.0), axis=1, keepdims=True
    )
    spread_t = jnp.where(iota((pair, rows), 1) // heads == iota((pair, rows), 0), 1.0, 0.0)
    code_lanes = nn_dot(code_b.astype(BF16), spread_t.astype(BF16))[0:1, :]
    full_lanes = code_lanes * heads + (iota((1, rows), 1) % heads).astype(F32)
    full_col = code_col * heads + (iota((rows, 1), 0) % heads).astype(F32)

    def slot_code(shape, dim):
        i = iota(shape, dim)
        k = i // hb
        o = jnp.where(k % 2 == 1, (k + 1) // 2, n - k // 2)
        t = (z + o) % n
        s = (i // heads) % slots
        return ((t * CAP + 2 * s + c) * heads + i % heads).astype(F32)

    slot_rows = slot_code((n * hb, 1), 0)
    slot_lanes = slot_code((1, n * hb), 1)
    gmat[...] = jnp.where(full_col == slot_lanes, 1.0, 0.0).astype(BF16)

    loads[0].wait()
    pack = jnp.where(slot_rows == full_lanes, 1.0, 0.0).astype(BF16)
    packed = nn_dot(pack, qv[...]).astype(BF16)
    qs[...] = packed.reshape(n, hb, hd)
    qr[0] = packed[0:hb]

    loads[1].wait()
    loads[2].wait()
    pl.semaphore_wait(barrier, n)

    q_copies = []
    for k in range(1, n):
        back = at(-order[k])
        copy = pltpu.make_async_remote_copy(
            src_ref=qs.at[k],
            dst_ref=qr.at[back],
            send_sem=q_send.at[k],
            recv_sem=q_recv.at[back],
            device_id=kv_dev(order[k]),
            device_id_type=MESH,
        )
        q_copies.append((k, back, copy))
    q_by_recv = {back: copy for k, back, copy in q_copies}

    def ring_copy(which, direction, j):
        buf = (kall, vall)[which]
        sign = 1 if direction == 0 else -1
        return pltpu.make_async_remote_copy(
            src_ref=buf.at[at(-sign * j)],
            dst_ref=buf.at[at(-sign * (j + 1))],
            send_sem=ring_send.at[which, direction, j],
            recv_sem=ring_recv.at[which, direction, j],
            device_id=kv_dev(sign),
            device_id_type=MESH,
        )

    ring = {}

    def ring_start(j):
        for which in range(2):
            for direction in range(2):
                if j == half - 1 and which != direction:
                    continue
                copy = ring_copy(which, direction, j)
                copy.start()
                ring[which, direction, j] = copy

    def ring_arrive(j):
        for which in range(2):
            for direction in range(2):
                if (which, direction, j) in ring:
                    ring[which, direction, j].wait_recv()

    ring_start(0)
    for _, _, copy in q_copies:
        copy.start()

    t_copies = []
    for i, (src, dst) in enumerate(((tk_hbm, tk), (tv_hbm, tv))):
        copy = pltpu.make_async_remote_copy(
            src_ref=src,
            dst_ref=dst.at[1],
            send_sem=t_send.at[i],
            recv_sem=t_recv.at[i],
            device_id=partner,
            device_id_type=MESH,
        )
        copy.start()
        t_copies.append(copy)

    def sys_step(first, count, start):
        keys = kall[first : first + count].reshape(count * kall.shape[1], hd)
        vals = vall[first : first + count].reshape(count * kall.shape[1], hd)
        s = nt_dot(qv[...], keys) * unit
        top = jnp.max(s, axis=1, keepdims=True)
        if start:
            m = top
        else:
            old = sys_m[...][:, 0:1]
            m = jnp.maximum(old, top)
        p = jnp.exp2(s - m)
        part = jnp.sum(p, axis=1, keepdims=True)
        num = nn_dot(p.astype(BF16), vals)
        if start:
            sys_l[...] = jnp.broadcast_to(part, (rows, hd))
            sys_acc[...] = num
        else:
            keep = jnp.exp2(old - m)
            sys_l[...] = sys_l[...] * keep + part
            sys_acc[...] = sys_acc[...] * keep + num
        sys_m[...] = jnp.broadcast_to(m, (rows, hd))

    two = 2 * heads

    def suffix_pair(i):
        upper = iota((two, 1), 0) < heads
        base = pl.multiple_of(c * own + i * two, two)
        q2 = qv[pl.ds(base, two), :]
        s = jnp.where(upper, nt_dot(q2, uk[2 * i]), nt_dot(q2, uk[2 * i + 1])) * unit
        limit = jnp.where(upper, len_ref[2 * i], len_ref[2 * i + 1])
        usable = iota((two, suf), 1) < limit
        s = jnp.where(usable, s, NEGATIVE)
        m = jnp.max(s, axis=1, keepdims=True)
        p = jnp.where(usable, jnp.exp2(s - m), 0.0)
        total = jnp.sum(p, axis=1, keepdims=True)
        pb = p.astype(BF16)
        num = jnp.where(upper, nn_dot(pb, uv[2 * i]), nn_dot(pb, uv[2 * i + 1]))
        suf_o[i * two : (i + 1) * two, :] = num / total
        suf_l[i * two : (i + 1) * two, :] = jnp.broadcast_to(m + jnp.log2(total), (two, hd))

    chunk = 512
    r_copies = []

    def task_group(first, count):
        height = count * hb
        for k in range(first, first + count):
            if k > 0:
                q_by_recv[k].wait_recv()
        query = qr[first : first + count].reshape(height, hd)
        top = None
        for b in range(2):
            for i in range(task_half // chunk):
                s = nt_dot(query, tk[b, i * chunk : (i + 1) * chunk, :]) * unit
                base = b * task_half + i * chunk
                scores[0:height, base : base + chunk] = s
                high = jnp.max(s, axis=1, keepdims=True)
                top = high if top is None else jnp.maximum(top, high)
        total = jnp.zeros((height, 1), F32)
        num = jnp.zeros((height, hd), F32)
        for b in range(2):
            for i in range(task_half // chunk):
                base = b * task_half + i * chunk
                p = jnp.exp2(scores[0:height, base : base + chunk] - top)
                total = total + jnp.sum(p, axis=1, keepdims=True)
                num = num + nn_dot(p.astype(BF16), tv[b, i * chunk : (i + 1) * chunk, :])
        result = (num / total).astype(BF16)
        level = jnp.broadcast_to(top + jnp.log2(total), (height, hd))
        for g in range(count):
            k = first + g
            back = at(-order[k])
            block = result[g * hb : (g + 1) * hb]
            lane = iota((hb, hd), 1) == iota((hb, hd), 0) + hb * (back % per)
            line = jnp.sum(
                jnp.where(lane, level[g * hb : (g + 1) * hb], 0.0), axis=0, keepdims=True
            )
            if k == 0:
                rr[0] = block
                sr[0] = line
                continue
            rs[k] = block
            ss[k] = line
            for src, dst, send, recv in ((rs, rr, r_send, r_recv), (ss, sr, s_send, s_recv)):
                copy = pltpu.make_async_remote_copy(
                    src_ref=src.at[k],
                    dst_ref=dst.at[back],
                    send_sem=send.at[k],
                    recv_sem=recv.at[back],
                    device_id=kv_dev(order[k]),
                    device_id_type=MESH,
                )
                copy.start()
                r_copies.append(copy)

    sys_step(0, 1, True)
    loads[3].wait()
    loads[4].wait()
    pairs_left = list(range(own_seqs // 2))
    groups = [(g * half, half) for g in range(2)]
    group_steps = {max(1, half // 2 - 1): 0, max(2, half // 2 + 1): 1}
    for j in range(1, half + 1):
        ring_arrive(j - 1)
        if j < half:
            ring_start(j)
        if j < half:
            sys_step(2 * j - 1, 2, False)
        else:
            sys_step(n - 1, 1, False)
        for _ in range(-(-(own_seqs // 2) // half)):
            if pairs_left:
                suffix_pair(pairs_left.pop(0))
        if j in group_steps:
            if group_steps[j] == 0:
                loads[5].wait()
                loads[6].wait()
                for copy in t_copies:
                    copy.wait_recv()
            task_group(*groups[group_steps[j]])

    for copy in r_copies:
        copy.wait_recv()
    g = gmat[...]
    task_o = nn_dot(g, rr[...].reshape(n * hb, hd))
    weighted = jnp.zeros((rows, hd), F32)
    for b in range(n // per):
        line = jnp.sum(sr[b * per : (b + 1) * per].reshape(per, hd), axis=0, keepdims=True)
        weighted = weighted + g[:, b * hd : (b + 1) * hd].astype(F32) * line
    task_l = jnp.sum(weighted, axis=1, keepdims=True)
    code_i = code_col.astype(jnp.int32)
    mine = code_i % 2 == c
    task_l = jnp.where(mine, task_l, NEGATIVE)
    old = sys_m[...]
    m = jnp.maximum(old, task_l)
    keep = jnp.exp2(old - m)
    gain = jnp.exp2(task_l - m)
    sys_acc[...] = sys_acc[...] * keep + task_o * gain
    den = sys_l[...] * keep + gain
    left_lanes = iota((rows, hd), 1) < hd // 2
    sys_m[...] = jnp.where(left_lanes, m, den)

    theirs = pl.ds(pl.multiple_of((1 - c) * own, own), own)
    ours = pl.ds(pl.multiple_of(c * own, own), own)
    xs[0] = sys_acc[theirs, :]
    xs[1] = sys_m[theirs, :]
    cross = []
    for i in range(2):
        copy = pltpu.make_async_remote_copy(
            src_ref=xs.at[i],
            dst_ref=xr.at[i],
            send_sem=x_send.at[i],
            recv_sem=x_recv.at[i],
            device_id=partner,
            device_id_type=MESH,
        )
        copy.start()
        cross.append(copy)
    a_num = sys_acc[ours, :]
    a_stat = sys_m[ours, :]
    u_o = suf_o[...]
    u_l = suf_l[...][:, 0:1]
    for copy in cross:
        copy.wait_recv()
    b_num = xr[0]
    b_stat = xr[1]
    a_m, a_d = a_stat[:, 0:1], a_stat[:, hd - 1 : hd]
    b_m, b_d = b_stat[:, 0:1], b_stat[:, hd - 1 : hd]
    m = jnp.maximum(jnp.maximum(a_m, b_m), u_l)
    fa, fb, fu = jnp.exp2(a_m - m), jnp.exp2(b_m - m), jnp.exp2(u_l - m)
    den = a_d * fa + b_d * fb + fu
    out_ref[...] = ((a_num * fa + b_num * fb + u_o * fu) / den).astype(out_ref.dtype)

    for copy in ring.values():
        copy.wait_send()
    for _, _, copy in q_copies:
        copy.wait_send()
    for copy in t_copies + r_copies + cross:
        copy.wait_send()


def body(
    queries,
    sys_keys,
    sys_values,
    task_keys,
    task_values,
    suffix_keys,
    suffix_values,
    task_ids,
    suffix_len,
):
    n = lax.axis_size("kv")
    pair, heads, hd = queries.shape
    rows = pair * heads
    shard = sys_keys.shape[1]
    task_half = task_keys.shape[2]
    own_seqs, _, suf, _ = suffix_keys.shape
    own = own_seqs * heads
    half = n // 2
    hb = CAP // 2 * heads
    any_space = pl.BlockSpec(memory_space=pl.ANY)
    vmem = pl.BlockSpec(memory_space=pltpu.VMEM)
    dma = pltpu.SemaphoreType.DMA
    out = pl.pallas_call(
        functools.partial(kernel, n, heads),
        out_shape=jax.ShapeDtypeStruct((own, hd), jnp.bfloat16),
        in_specs=[any_space] * 7 + [vmem, pl.BlockSpec(memory_space=pltpu.SMEM)],
        out_specs=vmem,
        scratch_shapes=[
            pltpu.VMEM((rows, hd), BF16),
            pltpu.VMEM((n, shard, hd), BF16),
            pltpu.VMEM((n, shard, hd), BF16),
            pltpu.VMEM((2, task_half, hd), BF16),
            pltpu.VMEM((2, task_half, hd), BF16),
            pltpu.VMEM((own_seqs, suf, hd), BF16),
            pltpu.VMEM((own_seqs, suf, hd), BF16),
            pltpu.VMEM((n, hb, hd), BF16),
            pltpu.VMEM((n, hb, hd), BF16),
            pltpu.VMEM((n, hb, hd), BF16),
            pltpu.VMEM((n, hb, hd), BF16),
            pltpu.VMEM((n, 1, hd), F32),
            pltpu.VMEM((n, 1, hd), F32),
            pltpu.VMEM((rows, n * hb), BF16),
            pltpu.VMEM((half * hb, 2 * task_half), F32),
            pltpu.VMEM((rows, hd), F32),
            pltpu.VMEM((rows, hd), F32),
            pltpu.VMEM((rows, hd), F32),
            pltpu.VMEM((own, hd), F32),
            pltpu.VMEM((own, hd), F32),
            pltpu.VMEM((2, own, hd), F32),
            pltpu.VMEM((2, own, hd), F32),
            dma((7,)),
            dma((2, 2, half)),
            dma((2, 2, half)),
            dma((n,)),
            dma((n,)),
            dma((n,)),
            dma((n,)),
            dma((n,)),
            dma((n,)),
            dma((2,)),
            dma((2,)),
            dma((2,)),
            dma((2,)),
        ],
        compiler_params=pltpu.CompilerParams(
            collective_id=0, has_side_effects=True, vmem_limit_bytes=56 * 1024 * 1024
        ),
        name="cascade",
    )(
        queries.reshape(rows, hd),
        sys_keys.reshape(shard, hd),
        sys_values.reshape(shard, hd),
        task_keys.reshape(task_half, hd),
        task_values.reshape(task_half, hd),
        suffix_keys.reshape(own_seqs, suf, hd),
        suffix_values.reshape(own_seqs, suf, hd),
        task_ids.reshape(1, pair),
        suffix_len,
    )
    return out.reshape(own_seqs, heads, hd)


def solution(mesh):
    in_specs = (
        P(("replica", "kv"), "head", None),
        P(("replica", "head"), ("kv", "sub"), None),
        P(("replica", "head"), ("kv", "sub"), None),
        P(("replica", "kv"), "head", "sub", None),
        P(("replica", "kv"), "head", "sub", None),
        P(("replica", "kv", "sub"), "head", None, None),
        P(("replica", "kv", "sub"), "head", None, None),
        P(("replica", "kv")),
        P(("replica", "kv", "sub")),
    )
    out_specs = P(("replica", "kv", "sub"), "head", None)
    return jax.shard_map(body, mesh=mesh, in_specs=in_specs, out_specs=out_specs, check_vma=False)
```

```python
import functools
import math

import jax
import jax.numpy as jnp
from jax import lax
from jax.experimental import pallas as pl
from jax.experimental.pallas import tpu as pltpu
from jax.sharding import PartitionSpec as P

CAP = 8
NEGATIVE = -1e30
RING_ORDERS = [28518, 27199, 22895, 19710, 21998, 26525, 22453, 27891, 29613, 24405, 32398, 30166, 24409, 16242, 30692, 32736]
MESH = pl.DeviceIdType.MESH
F32 = jnp.float32
BF16 = jnp.bfloat16


def nt_dot(a, b):
    return lax.dot_general(a, b, (((1,), (1,)), ((), ())), preferred_element_type=F32)


def nn_dot(a, b):
    return lax.dot_general(a, b, (((1,), (0,)), ((), ())), preferred_element_type=F32)


def iota(shape, dim):
    return lax.broadcasted_iota(jnp.int32, shape, dim)


def kernel(
    n,
    heads,
    q_hbm,
    sk_hbm,
    sv_hbm,
    tk_hbm,
    tv_hbm,
    uk_hbm,
    uv_hbm,
    ids_hbm,
    len_hbm,
    out_ref,
    qv,
    kall,
    vall,
    tk,
    tv,
    uk,
    uv,
    ids_ref,
    len_ref,
    qs,
    qr,
    rs,
    rr,
    ss,
    sr,
    gmat,
    scores,
    part_m,
    part_l,
    part_num,
    suf_l,
    suf_o,
    xs,
    xr,
    outv,
    local_sem,
    ring_send,
    ring_recv,
    q_send,
    q_recv,
    r_send,
    r_recv,
    s_send,
    s_recv,
    t_send,
    t_recv,
    x_send,
    x_recv,
    k_send,
    k_recv,
    mate_sem,
    in_sem,
    right_sem,
    left_sem,
):
    z = lax.axis_index("kv")
    c = lax.axis_index("sub")
    half = n // 2
    rows, hd = q_hbm.shape
    pair = rows // heads
    own = rows // 2
    own_seqs, suf, _ = uk_hbm.shape
    task_half = tk_hbm.shape[0]
    hb = CAP * heads
    per = hd // hb
    unit = math.log2(math.e) / math.sqrt(hd)

    order = [0]
    for d in range(1, half):
        order += [d, n - d]
    order.append(half)
    place = {o: k for k, o in enumerate(order)}

    def at(offset):
        return place[offset % n]

    def kv_dev(offset):
        return {"kv": lax.rem(z + (offset % n), n)}

    partner = {"sub": 1 - c}

    def remote(src, dst, send, recv, device):
        return pltpu.make_async_remote_copy(
            src_ref=src,
            dst_ref=dst,
            send_sem=send,
            recv_sem=recv,
            device_id=device,
            device_id_type=MESH,
        )

    def load(i, src, dst):
        return pltpu.make_async_copy(src, dst, local_sem.at[i])

    load_q = load(0, q_hbm, qv)
    load_len = load(1, len_hbm, len_ref)
    load_uk = load(2, uk_hbm, uk)
    load_uv = load(3, uv_hbm, uv)
    load_k = load(4, sk_hbm, kall.at[0, 1])
    load_v = load(5, sv_hbm, vall.at[0, 1])
    load_ids = load(4, ids_hbm, ids_ref)
    load_tk = load(5, tk_hbm, tk.at[0])
    load_tv = load(6, tv_hbm, tv.at[0])
    load_k0 = load(7, sk_hbm, kall.at[0, 0])
    load_v0 = load(8, sv_hbm, vall.at[0, 0])

    t_copies = [
        remote(src, dst.at[1], t_send.at[i], t_recv.at[i], partner)
        for i, (src, dst) in enumerate(((tk_hbm, tk), (tv_hbm, tv)))
    ]
    k_copies = [
        remote(buf.at[0, 0], buf.at[0, 0], k_send.at[i], k_recv.at[i], partner)
        for i, buf in enumerate((kall, vall))
    ]
    barrier = pltpu.get_barrier_semaphore()

    two = 2 * heads

    def suffix_pair(i):
        upper = iota((two, 1), 0) < heads
        base = pl.multiple_of(c * own + i * two, two)
        q2 = qv[pl.ds(base, two), :]
        s = jnp.where(upper, nt_dot(q2, uk[2 * i]), nt_dot(q2, uk[2 * i + 1])) * unit
        limit = jnp.where(upper, len_ref[2 * i], len_ref[2 * i + 1])
        usable = iota((two, suf), 1) < limit
        s = jnp.where(usable, s, NEGATIVE)
        m = jnp.max(s, axis=1, keepdims=True)
        p = jnp.where(usable, jnp.exp2(s - m), 0.0)
        total = jnp.sum(p, axis=1, keepdims=True)
        pb = p.astype(BF16)
        num = jnp.where(upper, nn_dot(pb, uv[2 * i]), nn_dot(pb, uv[2 * i + 1]))
        spot = pl.ds(pl.multiple_of(i * two, two), two)
        suf_o[spot, :] = num / total
        suf_l[spot, :] = jnp.broadcast_to(m + jnp.log2(total), (two, hd))

    def suffix_loads():
        load_len.wait()
        load_uk.wait()
        load_uv.wait()

    def suffixes():
        suffix_loads()

        @pl.loop(0, own_seqs // 2)
        def _(i):
            suffix_pair(i)

    left_lanes = iota((rows, hd), 1) < hd // 2

    reach = (n // 3, n - 1 - n // 3)

    def ring_copy(which, core, direction, j):
        buf = (kall, vall)[which]
        sign = 1 if direction == 0 else -1
        return remote(
            buf.at[(-sign * j) % n, core],
            buf.at[(-sign * (j + 1)) % n, core],
            ring_send.at[which],
            ring_recv.at[which, core, (-sign * (j + 1)) % n],
            kv_dev(sign),
        )

    ring = {
        (which, core, direction, j): ring_copy(which, core, direction, j)
        for which in range(2)
        for core in range(2)
        for direction in range(2)
        for j in range(1)
    }

    def ring_first(core, direction):
        for which in range(2):
            ring[which, core, direction, 0].start()

    def ring_open():
        load_k.wait()
        load_v.wait()
        for core in (1, 0):
            if core == 0:
                for copy in k_copies:
                    copy.wait_recv()

            @pl.when(z > 0)
            def _():
                ring_first(core, 1)

            @pl.when(z == n - 1)
            def _():
                ring_first(core, 0)

        pl.when(z > 0)(load_q.wait)
        sys_step(kall[0], vall[0], True)
        @pl.when(z < n - 1)
        def _():
            pl.semaphore_wait(right_sem, 1)
            for core in (1, 0):
                ring_first(core, 0)

        @pl.when(z == 0)
        def _():
            pl.semaphore_wait(left_sem, 1)
            for core in (1, 0):
                ring_first(core, 1)

        pl.when(z > 0)(suffix_loads)

    def ring_orders():
        if n == len(RING_ORDERS):
            return RING_ORDERS
        gap, hop, wire = 2.7, 2.1, 1.4
        come = [gap * (n - 1) + 1.0] + [gap * i for i in range(1, n)]
        when = {(d, 0, i): come[i] for d in range(2) for i in range(n)}
        for j in range(1, n):
            for d in range(2):
                for i in range(n):
                    source = (i - 1) % n if d == 0 else (i + 1) % n
                    at_source = max(when[d, j - 1, source], come[source], come[i] if i else 0) + hop
                    when[d, j, i] = max(at_source, when[d, j - 1, i] + wire)
        masks = []
        for i in range(n):
            events = sorted((when[d, j, i], j, d) for d in range(2) for j in range(1, reach[d] + 1))
            masks.append(sum(d << k for k, (_, _, d) in enumerate(events)))
        return masks

    def slot(d, j):
        return d * j + (1 - d) * ((n - j) % n)

    def ring_moves(d, j):
        def piece(which, core, step):
            buf = (kall, vall)[which]
            return remote(
                buf.at[slot(d, step), core],
                buf.at[slot(d, step + 1), core],
                ring_send.at[which],
                ring_recv.at[which, core, slot(d, step + 1)],
                {"kv": lax.rem(z + 1 - 2 * d + n, n)},
            )

        for core in (1, 0):
            for which in range(2):
                piece(which, core, j - 1).wait_recv()

                @pl.when(j < d * reach[1] + (1 - d) * reach[0])
                def _():
                    piece(which, core, j).start()

    def sys_step(keys, vals, start):
        keys = keys.reshape(-1, hd)
        vals = vals.reshape(-1, hd)
        s = nt_dot(qv[...], keys) * unit
        top = jnp.max(s, axis=1, keepdims=True)
        if start:
            m = top
        else:
            old = part_m[...][:, 0:1]
            m = jnp.maximum(old, top)
        p = jnp.exp2(s - m)
        part = jnp.sum(p, axis=1, keepdims=True)
        num = nn_dot(p.astype(BF16), vals)
        if start:
            part_l[...] = jnp.broadcast_to(part, (rows, hd))
            part_num[...] = num
        else:
            keep = jnp.exp2(old - m)
            part_l[...] = part_l[...] * keep + part
            part_num[...] = part_num[...] * keep + num
        part_m[...] = jnp.broadcast_to(m, (rows, hd))

    @pl.when(c == 1)
    def _():
        @pl.when(z < n - 1)
        def _():
            pl.semaphore_signal(barrier, inc=1, device_id=kv_dev(1), device_id_type=MESH)

        @pl.when(z == 0)
        def _():
            pl.semaphore_signal(barrier, inc=1, device_id=kv_dev(-1), device_id_type=MESH)

        for copy in (load_k, load_v, load_q, load_len, load_uk, load_uv):
            copy.start()
        @pl.when(z == 0)
        def _():
            load_q.wait()
            suffixes()

        pl.semaphore_wait(barrier, 1 + (z + n - 1) // n + (z + 1) // n)
        pl.semaphore_signal(mate_sem, inc=1, device_id=partner, device_id_type=MESH)

        @pl.when(z > 0)
        def _():
            pl.semaphore_signal(right_sem, inc=1, device_id=kv_dev(-1), device_id_type=MESH)

        @pl.when(z == n - 1)
        def _():
            pl.semaphore_signal(left_sem, inc=1, device_id=kv_dev(1), device_id_type=MESH)

        for copy in t_copies:
            copy.start()
        ring_open()
        first_in = half
        mask = 0
        for i, value in enumerate(ring_orders()):
            mask = mask + jnp.where(z == i, value, 0)

        @pl.loop(0, half, init_carry=(jnp.int32(0), mask))
        def _(i, carry):
            lefts, bits = carry
            at_once = z < first_in
            paired = i < half - 1

            def event(e, lefts, bits):
                d = bits % 2
                j = d * (lefts + 1) + (1 - d) * (2 * i + e - lefts + 1)
                ring_moves(d, j)
                return slot(d, j), lefts + d, bits // 2

            first, lefts, bits = event(0, lefts, bits)

            @pl.when(paired)
            def _():
                second, _, _ = event(1, lefts, bits)

                @pl.when(at_once)
                def _():
                    sys_step(
                        jnp.concatenate([kall[first], kall[second]], axis=0),
                        jnp.concatenate([vall[first], vall[second]], axis=0),
                        False,
                    )

            @pl.when(jnp.logical_and(at_once, jnp.logical_not(paired)))
            def _():
                sys_step(kall[first], vall[first], False)

            lefts, bits = lefts + bits % 2, bits // 2

            @pl.when(jnp.logical_and(jnp.logical_and(z > 0, at_once), i < own_seqs // 2))
            def _():
                suffix_pair(i)

            return lefts, bits

        @pl.when(z >= first_in)
        def _():
            @pl.loop(1, half)
            def _(i):
                spot = pl.ds(2 * i - 1, 2)
                sys_step(kall[spot], vall[spot], False)

            @pl.loop(0, min(half, own_seqs // 2))
            def _(i):
                suffix_pair(i)

            sys_step(kall[n - 1], vall[n - 1], False)

        @pl.when(z > 0)
        def _():
            @pl.loop(half, max(own_seqs // 2, half))
            def _(i):
                suffix_pair(i)

        part_m[...] = jnp.where(left_lanes, part_m[...], part_l[...])

    v = z - 1 + (1 - (z + n - 1) // n) * (n - 1) + z // (n - 1)

    def nth(i):
        if i == 0:
            return v
        below = (v - i + n) // n
        lower = v - (i + 1) // 2 if i % 2 == 1 else i // 2 - 1
        return below * lower + (1 - below) * i

    def kv_of(k):
        return (k + 1) * (1 - k // (n - 2)) + (k // (n - 1)) * (n - 1)

    def dev(k):
        return {"kv": kv_of(k)}

    def q_copy(k):
        return remote(qs.at[k], qr.at[v], q_send.at[0], q_recv.at[v], dev(k))

    def q_arrival(k):
        return remote(qs.at[k], qr.at[k], q_send.at[0], q_recv.at[k], dev(k))

    def r_copy(k):
        return [
            remote(rs.at[k], rr.at[v], r_send.at[0], r_recv.at[0], dev(k)),
            remote(ss.at[k], sr.at[v], s_send.at[0], s_recv.at[0], dev(k)),
        ]

    others = pl.ds(0, n - 1)
    mate_dev = {"sub": 1 - c}
    q_all = remote(qs.at[others], qr.at[others], q_send.at[0], q_recv.at[0], mate_dev)
    r_all = [
        remote(rs.at[others], rr.at[others], r_send.at[0], r_recv.at[0], mate_dev),
        remote(ss.at[others], sr.at[others], s_send.at[0], s_recv.at[0], mate_dev),
    ]
    ring_all = [
        remote(
            buf.at[others], buf.at[others], ring_send.at[i], ring_recv.at[i, 0, 0], mate_dev
        )
        for i, buf in enumerate((kall, vall))
    ]

    chunk = 512

    def task_group(first, count):
        height = count * hb
        names = [nth(i) for i in range(first, first + count)]
        for i in range(count):
            if first + i > 0:
                q_arrival(names[i]).wait_recv()
        query = jnp.concatenate([qr[k] for k in names], axis=0)
        top = None
        for b in range(2):
            for i in range(task_half // chunk):
                s = nt_dot(query, tk[b, i * chunk : (i + 1) * chunk, :]) * unit
                base = b * task_half + i * chunk
                scores[0:height, base : base + chunk] = s
                high = jnp.max(s, axis=1, keepdims=True)
                top = high if top is None else jnp.maximum(top, high)
        total = jnp.zeros((height, 1), F32)
        num = jnp.zeros((height, hd), F32)
        for b in range(2):
            for i in range(task_half // chunk):
                base = b * task_half + i * chunk
                p = jnp.exp2(scores[0:height, base : base + chunk] - top)
                total = total + jnp.sum(p, axis=1, keepdims=True)
                num = num + nn_dot(p.astype(BF16), tv[b, i * chunk : (i + 1) * chunk, :])
        result = (num / total).astype(BF16)
        level = jnp.broadcast_to(top + jnp.log2(total), (height, hd))
        for g in range(count):
            k = names[g]
            block = result[g * hb : (g + 1) * hb]
            lane = iota((hb, hd), 1) == iota((hb, hd), 0) + hb * (v % per)
            line = jnp.sum(
                jnp.where(lane, level[g * hb : (g + 1) * hb], 0.0), axis=0, keepdims=True
            )
            if first + g == 0:
                rr[v] = block
                sr[v] = line
                continue
            rs[k] = block
            ss[k] = line
            for copy in r_copy(k):
                copy.start()

    near = 5

    def ask_above(first, last, rest):
        for k in range(first, last):
            chosen = k > v + near if rest else jnp.logical_and(k > v, k <= v + near)

            @pl.when(chosen)
            def _():
                pl.semaphore_wait(in_sem.at[k], 1)
                q_copy(k).start()

    def enter():
        @pl.when(v > 0)
        def _():
            pl.semaphore_wait(barrier, 1 + v // (n - 1))

        @pl.when(v < n - 2)
        def _():
            pl.semaphore_signal(barrier, inc=1, device_id=dev(v + 1), device_id_type=MESH)

        @pl.when(v == n - 3)
        def _():
            pl.semaphore_signal(barrier, inc=1, device_id=dev(n - 1), device_id_type=MESH)

        for i in range(1, n):

            @pl.when(i <= v)
            def _():
                pl.semaphore_signal(
                    in_sem.at[v], inc=1, device_id=dev(nth(i)), device_id_type=MESH
                )

    @pl.when(c == 0)
    def _():
        mate = {"sub": 1}
        pl.semaphore_signal(barrier, inc=1, device_id=mate, device_id_type=MESH)

        @pl.when(z == 0)
        def _():
            pl.semaphore_signal(barrier, inc=1, device_id=dev(n - 1), device_id_type=MESH)

        for copy in (load_ids, load_q, load_k0, load_v0, load_len, load_uk, load_uv, load_tk, load_tv):
            copy.start()

        def give_keys():
            pl.semaphore_wait(mate_sem, 1)
            load_k0.wait()
            load_v0.wait()
            for copy in k_copies:
                copy.start()

        pl.when(z == 0)(give_keys)
        enter()
        pl.when(z == n - 1)(give_keys)

        load_ids.wait()
        ids_row = ids_ref[...].astype(F32)
        ids_b = jnp.broadcast_to(ids_row, (pair, pair))
        eye = iota((pair, pair), 0) == iota((pair, pair), 1)
        ids_col = jnp.sum(jnp.where(eye, ids_b, 0.0), axis=1, keepdims=True)
        before = iota((pair, pair), 0) < iota((pair, pair), 1)
        same = jnp.logical_and(ids_col == ids_b, before)
        rank_row = jnp.sum(jnp.where(same, 1.0, 0.0), axis=0, keepdims=True)
        code_row = ids_row * CAP + rank_row
        code_b = jnp.broadcast_to(code_row, (pair, pair))
        spread = iota((rows, pair), 0) // heads == iota((rows, pair), 1)
        code_col = jnp.sum(
            jnp.where(spread, jnp.broadcast_to(code_row, (rows, pair)), 0.0), axis=1, keepdims=True
        )
        spread_t = jnp.where(iota((pair, rows), 1) // heads == iota((pair, rows), 0), 1.0, 0.0)
        code_lanes = nn_dot(code_b.astype(BF16), spread_t.astype(BF16))[0:1, :]
        full_lanes = code_lanes * heads + (iota((1, rows), 1) % heads).astype(F32)
        full_col = code_col * heads + (iota((rows, 1), 0) % heads).astype(F32)

        def slot_code(shape, dim):
            i = iota(shape, dim)
            return (kv_of(i // hb) * hb + i % hb).astype(F32)

        load_q.wait()
        pack = jnp.where(slot_code((n * hb, 1), 0) == full_lanes, 1.0, 0.0).astype(BF16)
        packed = nn_dot(pack, qv[...]).astype(BF16)
        qs[...] = packed.reshape(n, hb, hd)
        for i in reversed(range(1, n)):

            @pl.when(i <= v)
            def _():
                q_copy(nth(i)).start()

        pl.when(v < n - 2)(give_keys)
        qr[v] = qs[v]
        gmat[...] = jnp.where(full_col == slot_code((1, n * hb), 1), 1.0, 0.0).astype(BF16)
        pl.when(v < n - 2)(suffixes)
        ask_above(1, n, False)
        load_tk.wait()
        load_tv.wait()
        for copy in t_copies:
            copy.wait_recv()
        done, asked = 0, 1
        while done < n:
            count = half // 2 if done < half else max(half // 4, 1)
            ahead = min(done + count + 4, n)
            ask_above(asked, ahead, True)
            asked = ahead
            if done == 0:
                pl.when(v >= n - 2)(suffixes)
            task_group(done, count)
            done += count

        for copy in r_all:
            copy.wait_recv()

        g = gmat[...]
        part_num[...] = nn_dot(g, rr[...].reshape(n * hb, hd))
        weighted = jnp.zeros((rows, hd), F32)
        for b in range(n // per):
            line = jnp.sum(sr[b * per : (b + 1) * per].reshape(per, hd), axis=0, keepdims=True)
            weighted = weighted + g[:, b * hd : (b + 1) * hd].astype(F32) * line
        task_l = jnp.sum(weighted, axis=1, keepdims=True)
        part_m[...] = jnp.where(left_lanes, task_l, 1.0)

    theirs = pl.ds(pl.multiple_of((1 - c) * own, own), own)
    ours = pl.ds(pl.multiple_of(c * own, own), own)
    xs[0] = part_num[theirs, :]
    xs[1] = part_m[theirs, :]
    cross = [remote(xs.at[i], xr.at[i], x_send.at[i], x_recv.at[i], partner) for i in range(2)]
    for copy in cross:
        copy.start()
    a_num = part_num[ours, :]
    a_stat = part_m[ours, :]
    u_o = suf_o[...]
    u_l = suf_l[...][:, 0:1]
    for copy in cross:
        copy.wait_recv()
    b_num = xr[0]
    b_stat = xr[1]
    a_m, a_d = a_stat[:, 0:1], a_stat[:, hd - 1 : hd]
    b_m, b_d = b_stat[:, 0:1], b_stat[:, hd - 1 : hd]
    m = jnp.maximum(jnp.maximum(a_m, b_m), u_l)
    fa, fb, fu = jnp.exp2(a_m - m), jnp.exp2(b_m - m), jnp.exp2(u_l - m)
    den = a_d * fa + b_d * fb + fu
    outv[...] = ((a_num * fa + b_num * fb + u_o * fu) / den).astype(BF16)
    give = pltpu.make_async_copy(outv, out_ref, local_sem.at[0])
    give.start()

    for copy in cross:
        copy.wait_send()
    give.wait()

    @pl.when(c == 1)
    def _():
        for copy in ring_all + t_copies:
            copy.wait_send()

    @pl.when(c == 0)
    def _():
        for copy in k_copies + [q_all] + r_all:
            copy.wait_send()


def body(
    queries,
    sys_keys,
    sys_values,
    task_keys,
    task_values,
    suffix_keys,
    suffix_values,
    task_ids,
    suffix_len,
):
    n = lax.axis_size("kv")
    pair, heads, hd = queries.shape
    rows = pair * heads
    shard = sys_keys.shape[1]
    task_half = task_keys.shape[2]
    own_seqs, _, suf, _ = suffix_keys.shape
    own = own_seqs * heads
    half = n // 2
    hb = CAP * heads
    any_space = pl.BlockSpec(memory_space=pl.ANY)
    dma = pltpu.SemaphoreType.DMA
    out = pl.pallas_call(
        functools.partial(kernel, n, heads),
        out_shape=jax.ShapeDtypeStruct((own, hd), jnp.bfloat16),
        in_specs=[any_space] * 9,
        out_specs=any_space,
        scratch_shapes=[
            pltpu.VMEM((rows, hd), BF16),
            pltpu.VMEM((n, 2, shard, hd), BF16),
            pltpu.VMEM((n, 2, shard, hd), BF16),
            pltpu.VMEM((2, task_half, hd), BF16),
            pltpu.VMEM((2, task_half, hd), BF16),
            pltpu.VMEM((own_seqs, suf, hd), BF16),
            pltpu.VMEM((own_seqs, suf, hd), BF16),
            pltpu.VMEM((1, pair), jnp.int32),
            pltpu.SMEM((own_seqs,), jnp.int32),
            pltpu.VMEM((n, hb, hd), BF16),
            pltpu.VMEM((n, hb, hd), BF16),
            pltpu.VMEM((n, hb, hd), BF16),
            pltpu.VMEM((n, hb, hd), BF16),
            pltpu.VMEM((n, 1, hd), F32),
            pltpu.VMEM((n, 1, hd), F32),
            pltpu.VMEM((rows, n * hb), BF16),
            pltpu.VMEM((half // 2 * hb, 2 * task_half), F32),
            pltpu.VMEM((rows, hd), F32),
            pltpu.VMEM((rows, hd), F32),
            pltpu.VMEM((rows, hd), F32),
            pltpu.VMEM((own, hd), F32),
            pltpu.VMEM((own, hd), F32),
            pltpu.VMEM((2, own, hd), F32),
            pltpu.VMEM((2, own, hd), F32),
            pltpu.VMEM((own, hd), BF16),
            dma((9,)),
            dma((2,)),
            dma((2, 2, n)),
            dma((1,)),
            dma((n,)),
            dma((1,)),
            dma((1,)),
            dma((1,)),
            dma((1,)),
            dma((2,)),
            dma((2,)),
            dma((2,)),
            dma((2,)),
            dma((2,)),
            dma((2,)),
            pltpu.SemaphoreType.REGULAR,
            pltpu.SemaphoreType.REGULAR((n,)),
            pltpu.SemaphoreType.REGULAR,
            pltpu.SemaphoreType.REGULAR,
        ],
        compiler_params=pltpu.CompilerParams(
            collective_id=0, has_side_effects=True, vmem_limit_bytes=56 * 1024 * 1024
        ),
        name="cascade",
    )(
        queries.reshape(rows, hd),
        sys_keys.reshape(shard, hd),
        sys_values.reshape(shard, hd),
        task_keys.reshape(task_half, hd),
        task_values.reshape(task_half, hd),
        suffix_keys.reshape(own_seqs, suf, hd),
        suffix_values.reshape(own_seqs, suf, hd),
        task_ids.reshape(1, pair),
        suffix_len,
    )
    return out.reshape(own_seqs, heads, hd)


def solution(mesh):
    in_specs = (
        P(("replica", "kv"), "head", None),
        P(("replica", "head"), ("kv", "sub"), None),
        P(("replica", "head"), ("kv", "sub"), None),
        P(("replica", "kv"), "head", "sub", None),
        P(("replica", "kv"), "head", "sub", None),
        P(("replica", "kv", "sub"), "head", None, None),
        P(("replica", "kv", "sub"), "head", None, None),
        P(("replica", "kv")),
        P(("replica", "kv", "sub")),
    )
    out_specs = P(("replica", "kv", "sub"), "head", None)
    return jax.shard_map(body, mesh=mesh, in_specs=in_specs, out_specs=out_specs, check_vma=False)
```
